512 devices in a mesh: row: 32 (over y, z_lo), col: 16 (over z_hi, x, core).
Axes of the slice: x: 4, y: 8, z: 8 (z_hi: 2, z_lo: 4; z = z_hi * 4 + z_lo), core: 2. Of those that a mesh axis runs over, the one named last changes fastest.
Arguments:
- spectra: bfloat16 [4096, 16, 128], P(('row', 'col')), may hold values from -4 to 4
- window_flags: int32 [4096, 64], P(('row', 'col')), may hold values 0 or 1
- pair_mask: int32 [4096, 4096], P('row', 'col'), may hold values 0 or 1
- misfit_weight: bfloat16 [16, 4096, 4096], P(None, 'row', 'col'), may hold values from 0.0099487305 to 0.099609375
- observed: bfloat16 [2, 16, 4096, 4096], P(None, None, 'row', 'col'), may hold values from -6 to 6
Outputs:
- grad_first: bfloat16 [4096, 16, 128], P(('row', 'col'))
- grad_second: bfloat16 [16, 256, 16, 128], P('col', 'row')
The draws below stay inside these ranges and needn't reach their ends.
All inputs are finite; a program needn't handle non-finite values. No bound on the sum of `window_flags` or of `pair_mask` on one device may be relied on, other than what follows from the above.
Results may differ from the reference program's by a relative error of at most 0.019.
Values may be sent and summed in bfloat16 or wider, within the bound.
A program may use at most 64 MiB of HBM per device.

```python
import math
import jax
import jax.numpy as jnp
from jax import lax

ROW_BLOCK = 128
FREQS = 16
WINDOWS = 64
STATIONS = 4096
N_ROW = 32
N_COL = 16


def with_ends(values, stream_key, smallest, largest):
    longest = values.shape.index(max(values.shape))
    spots = []
    for shift in (0, 1):
        where = [jax.random.randint(jax.random.fold_in(stream_key, axis), (), 0, length) for axis, length in enumerate(values.shape)]
        where[longest] = (where[longest] + shift) % values.shape[longest]
        spots.append(tuple(where))
    return values.at[spots[0]].set(smallest).at[spots[1]].set(largest)


def levels(stream_key, shape, split, low, high):
    def one(axis_at, parts):
        heights = jax.random.uniform(jax.random.fold_in(jax.random.fold_in(stream_key, 6), axis_at), (parts,), jnp.float32, low / len(split), high / len(split))
        return jnp.repeat(jnp.exp(heights), shape[axis_at] // parts).reshape((-1,) + (1,) * (len(shape) - axis_at - 1))

    gain = one(*split[0])
    for cut in split[1:]:
        gain = gain * one(*cut)
    return gain


def noise(own_key, dims, deviation, bound, pieces=(), held_as=jnp.bfloat16):
    array = jax.random.normal(own_key, dims, jnp.float32) * deviation
    if len(pieces) > 0:
        array = levels(own_key, dims, pieces, -0.22, 0.18) * array
    return jnp.clip(array, min=-bound, max=bound).astype(held_as)


def setup_inputs(seed: int = 0) -> dict:
    seeds = jax.random.split(jax.random.key(seed), 6)
    spectra = noise(seeds[0], (STATIONS, FREQS, 2 * WINDOWS), 0.3, 4.0, ((0, 512),))
    window_flags = with_ends((jax.random.randint(seeds[1], (STATIONS, WINDOWS), 0, 4) < 3).astype(jnp.int32), jax.random.fold_in(seeds[1], 1), 0, 1)
    pair_mask = with_ends((jax.random.randint(seeds[2], (STATIONS, STATIONS), 0, 5) < 3).astype(jnp.int32), jax.random.fold_in(seeds[2], 1), 0, 1)
    misfit_weight = jnp.clip(jnp.exp(math.log(0.099609375) - 2.3038113 * jax.random.uniform(seeds[3], (FREQS, STATIONS, STATIONS), jnp.float32) ** levels(seeds[3], (FREQS, STATIONS, STATIONS), ((1, 32), (2, 16)), -0.2, 0.2)), 0.0099487305, 0.099609375).astype(jnp.bfloat16)
    observed = noise(seeds[4], (2, FREQS, STATIONS, STATIONS), 1.0, 6.0, ((2, 32), (3, 16)))
    return dict(spectra=spectra, window_flags=window_flags, pair_mask=pair_mask, misfit_weight=misfit_weight, observed=observed)


def reference(spectra, window_flags, pair_mask, misfit_weight, observed):
    half_width = spectra.shape[2] // 2
    flag_value = window_flags.astype(jnp.float32)
    flag_both = jnp.concatenate([flag_value, flag_value], axis=1)
    flagged = (spectra.astype(jnp.float32) * flag_both[:, None, :]).astype(jnp.bfloat16)
    flagged_wide = flagged.astype(jnp.float32)
    swapped = jnp.concatenate([-flagged_wide[..., half_width:], flagged_wide[..., :half_width]], axis=-1)
    col_stack = jnp.stack([flagged_wide, swapped])
    row_stack = jnp.stack([flagged_wide, -swapped])
    col_block = STATIONS // N_COL
    mask_wide = pair_mask.astype(jnp.float32)
    weight_wide = misfit_weight.astype(jnp.float32)
    observed_wide = observed.astype(jnp.float32)
    split_col = col_stack.reshape(2, N_COL, col_block, FREQS, 2 * WINDOWS)

    def one_block(accum_second, block_index):
        first_row = (block_index * ROW_BLOCK).astype(jnp.int32)
        row_part = lax.dynamic_slice_in_dim(flagged_wide, first_row, ROW_BLOCK, 0)
        row_pair = lax.dynamic_slice_in_dim(row_stack, first_row, ROW_BLOCK, 1)
        mask_part = lax.dynamic_slice_in_dim(mask_wide, first_row, ROW_BLOCK, 0)
        weight_part = lax.dynamic_slice_in_dim(weight_wide, first_row, ROW_BLOCK, 1)
        observed_part = lax.dynamic_slice_in_dim(observed_wide, first_row, ROW_BLOCK, 2)
        cross_spec = jnp.einsum('ifk,cjfk->cfij', row_part, col_stack, precision=lax.Precision.HIGHEST)
        residual = (mask_part[None, None] * weight_part[None] * (cross_spec - observed_part)).astype(jnp.bfloat16)
        residual = lax.optimization_barrier(residual).astype(jnp.float32)
        split_res = residual.reshape(2, FREQS, ROW_BLOCK, N_COL, col_block)
        first_terms = jnp.einsum('cfinj,cnjfk->nifk', split_res, split_col, precision=lax.Precision.HIGHEST)
        first_terms = lax.optimization_barrier(first_terms.astype(jnp.bfloat16)).astype(jnp.float32)
        first_grad = jnp.sum(first_terms, axis=0).astype(jnp.bfloat16)
        second_terms = jnp.einsum('cfij,cifk->jfk', residual, row_pair, precision=lax.Precision.HIGHEST)
        second_terms = lax.optimization_barrier(second_terms.astype(jnp.bfloat16)).astype(jnp.float32)
        return accum_second + second_terms, first_grad

    initial = jnp.zeros((STATIONS, FREQS, 2 * WINDOWS), jnp.float32)
    accum_second, firsts = lax.scan(one_block, initial, jnp.arange(N_ROW, dtype=jnp.int32))
    grad_first = firsts.reshape(STATIONS, FREQS, 2 * WINDOWS)
    grad_second = accum_second.astype(jnp.bfloat16).reshape(N_COL, col_block, FREQS, 2 * WINDOWS)
    return grad_first, grad_second
```

```python
import jax
import jax.numpy as jnp
from jax import lax
from jax.experimental import pallas as pl
from jax.experimental.pallas import tpu as pltpu
from jax.sharding import PartitionSpec as P

MESH = pl.DeviceIdType.MESH
BF = jnp.bfloat16
F32 = jnp.float32
F = 16
K = 128
CHIPS = 8
YS = 8
ZS = 4
HALF = F // 2
STREAMS = ((1, 0, 4), (-1, 1, 4), (1, 1, 3), (-1, 0, 3))
FIRST = (0, 4, 8, 11)
MESSAGES = 14


def shift_of(here, there):
    hi = lax.rem(here // 4 + there // 4, 2)
    dx = lax.rem(here - there + 8, 4)
    same = 4 - dx + 4 * (dx // 2)
    other = lax.rem(2 - dx + 8, 8)
    return hi * other + (1 - hi) * same


def chip_at(there, y):
    dy = lax.rem(y - there + 8, 8)
    hi = 1 - lax.rem(dy + 1, 8) // 4
    dx = lax.rem(hi * 2 + (1 - hi) * 4 - dy + 8, 4)
    return lax.rem(there // 4 + hi, 2) * 4 + lax.rem(there + dx, 4)


def kernel(
    spectra, flags, mask, weight, observed, grad_first, grad_second,
    spec_v, flag_v, mask_v, weight_v, obs_v, turn, mine, first, second,
    gf_own, gf_got, gf_sum, gf_in, gs_own, gs_got, gz_own, gz_in,
    load_sem, put_s, put_r, hi_s, hi_r, x_s, x_r, pair_s, pair_r, ring_s, ring_r,
    gp_s, gp_r, gx_s, gx_r, red_s, red_r, z_s, z_r,
):
    row = lax.axis_index("row")
    col = lax.axis_index("col")
    y, zl = row // ZS, lax.rem(row, ZS)
    chip, core = col // 2, lax.rem(col, 2)
    hi, x = chip // 4, lax.rem(chip, 4)

    def device(y, zl, chip, core):
        return (y * ZS + zl, chip * 2 + core)

    def step_y(n):
        return lax.rem(y + n + 2 * YS, YS)

    def remote(src, dst, send, recv, to):
        return pltpu.make_async_remote_copy(
            src_ref=src, dst_ref=dst, send_sem=send, recv_sem=recv, device_id=to, device_id_type=MESH
        )

    loads = [
        pltpu.make_async_copy(a, b, load_sem.at[n])
        for n, (a, b) in enumerate(
            ((spectra, spec_v), (flags, flag_v), (mask, mask_v), (weight, weight_v), (observed, obs_v))
        )
    ]
    for load in loads:
        load.start()

    barrier = pltpu.get_barrier_semaphore()
    partner = device(y, zl, chip, 1 - core)
    peers = [partner]
    peers += [device(y, zl, lax.rem(chip + n, CHIPS), core) for n in range(1, CHIPS)]
    peers += [device(step_y(n), zl, chip, core) for n in (1, -1)]
    peers += [device(y, lax.rem(zl + n, ZS), chip, core) for n in range(1, ZS)]
    giver = chip_at(chip, y)
    peers += [device(chip, 2 * core + b, giver, c) for b in range(2) for c in range(2)]
    for peer in peers:
        pl.semaphore_signal(barrier, inc=1, device_id=peer, device_id_type=MESH)

    loads[0].wait()
    loads[1].wait()
    turn[...] = spec_v[...].astype(F32).reshape(8 * F, K)
    flag = flag_v[...].astype(F32)
    flag = jnp.concatenate([flag, flag], axis=1)
    pieces = [(turn[pl.ds(f, 8, stride=F), :] * flag).astype(BF) for f in range(F)]
    for f in range(F):
        mine[f] = pieces[f]

    for c in range(2):

        @pl.when(core == c)
        def _():
            for f in range(F):
                first[chip, f, 8 * c : 8 * c + 8, :] = pieces[f]

    pl.semaphore_wait(barrier, len(peers))

    def eight(c):
        return pl.ds(pl.multiple_of(c * 8, 8), 8)

    to_y = lax.rem(y + shift_of(chip, y), YS)
    puts = []
    for n in range(ZS):
        puts.append(
            remote(
                mine,
                second.at[chip, :, lax.rem(zl, 2), eight(core), :],
                put_s.at[n],
                put_r.at[lax.rem(zl, 2) * 2 + core],
                device(to_y, lax.rem(zl + n, ZS), y, zl // 2),
            )
        )
        puts[-1].start()

    far = lax.rem(hi + 1, 2) * 4 + x
    cross_hi = remote(mine, first.at[chip, :, eight(core), :], hi_s, hi_r, device(y, zl, far, core))
    cross_hi.start()
    along_x = []
    for n in range(1, 4):
        to = device(y, zl, hi * 4 + lax.rem(x + n, 4), core)
        along_x.append(remote(mine, first.at[chip, :, eight(core), :], x_s.at[n - 1], x_r.at[n - 1], to))
        along_x[-1].start()

    for b in range(2):
        for c in range(2):
            n = b * 2 + c
            remote(mine, second.at[giver, :, b, 8 * c : 8 * c + 8, :], put_s.at[n], put_r.at[n], partner).wait_recv()

    def ring_copy(s, t):
        way, half, steps = STREAMS[s]
        block = second.at[chip_at(chip, step_y(-way * (t - 1))), half * HALF : half * HALF + HALF]
        n = FIRST[s] + t - 1
        return remote(block, block, ring_s.at[n], ring_r.at[n], device(step_y(way), zl, chip, core))

    def ring_arrival(s, t):
        way, half, steps = STREAMS[s]
        block = second.at[chip_at(chip, step_y(-way * t)), half * HALF : half * HALF + HALF]
        n = FIRST[s] + t - 1
        return remote(block, block, ring_s.at[n], ring_r.at[n], device(step_y(way), zl, chip, core))

    ring = []
    for s in range(4):
        ring.append(ring_copy(s, 1))
        ring[-1].start()

    remote(mine, first.at[far, :, eight(core), :], hi_s, hi_r, partner).wait_recv()
    for n in range(1, 4):
        to = device(y, zl, hi * 4 + lax.rem(x + n, 4), core)
        block = first.at[far, :, eight(core), :]
        along_x.append(remote(block, block, x_s.at[n + 2], x_r.at[n + 2], to))
        along_x[-1].start()

    def ring_step(t):
        for s in range(4):
            if t <= STREAMS[s][2]:
                ring_arrival(s, t - 1).wait_recv()
                ring.append(ring_copy(s, t))
                ring[-1].start()

    ring_step(2)

    pair = []
    for g in range(2):
        for n in range(1, 4):
            from_chip = (hi if g == 0 else lax.rem(hi + 1, 2)) * 4 + lax.rem(x - n + 4, 4)
            m = g * 3 + n - 1
            remote(mine, first.at[from_chip, :, eight(core), :], x_s.at[m], x_r.at[m], partner).wait_recv()
    block = first.at[:, :, eight(core), :]
    pair.append(remote(block, block, pair_s, pair_r, partner))
    pair[-1].start()

    ring_step(3)
    ring_step(4)
    other = first.at[:, :, eight(1 - core), :]
    remote(other, other, pair_s, pair_r, partner).wait_recv()
    for load in loads[2:]:
        load.wait()
    for s in range(4):
        ring_arrival(s, STREAMS[s][2]).wait_recv()

    lane = lax.broadcasted_iota(jnp.int32, (1, K), 1)
    sign = jnp.where(lane < K // 2, 1.0, -1.0).astype(F32)

    def one_frequency(f, carry):
        v = first[:, f].reshape(128, K)
        turned = (pltpu.roll(v.astype(F32), K // 2, 1) * sign).astype(BF)
        rows = jnp.concatenate([v, turned], axis=0)
        cols = jnp.concatenate([second[:, f, b].reshape(128, K) for b in range(2)], axis=0)
        cross = lax.dot_general(rows, cols, (((1,), (1,)), ((), ())), preferred_element_type=F32)
        scale = mask_v[...].astype(F32) * weight_v[f].astype(F32)
        residual = jnp.concatenate(
            [(scale * (cross[128 * c : 128 * c + 128] - obs_v[c, f].astype(F32))).astype(BF) for c in range(2)], axis=0
        )
        prod = jnp.dot(residual, cols, preferred_element_type=F32)
        gf = prod[:128] - pltpu.roll(prod[128:], K // 2, 1) * sign
        gf = gf.reshape(CHIPS, 2, 8, K)
        for c in range(2):
            gf_own[c, :, f] = gf[:, c].astype(BF)
        gs = lax.dot_general(residual, rows, (((0,), (0,)), ((), ())), preferred_element_type=F32)
        gs_own[:, f] = gs.reshape(YS, 32, K).astype(BF)
        return carry

    lax.fori_loop(0, F, one_frequency, 0)

    def half_of(ref, half):
        return ref.at[half * HALF : half * HALF + HALF]

    def red_copy(s, t):
        way, half, steps = STREAMS[s]
        n = FIRST[s] + t - 1
        src = half_of(gs_own.at[step_y(way * (steps - t + 1))], half)
        return remote(src, gs_got.at[n], red_s.at[n], red_r.at[n], device(step_y(way), zl, chip, core))

    red = []
    for s in range(4):
        red.append(red_copy(s, 1))
        red[-1].start()

    gpair = remote(gf_own.at[1 - core], gf_got, gp_s, gp_r, partner)
    gpair.start()

    def red_step(t):
        for s in range(4):
            way, half, steps = STREAMS[s]
            if t <= steps:
                n = FIRST[s] + t - 2
                red_copy(s, t - 1).wait_recv()
                acc = gs_own.at[step_y(way * (steps - t + 1))]
                span = slice(half * HALF, half * HALF + HALF)
                acc[span] = (acc[span].astype(F32) + gs_got[n].astype(F32)).astype(BF)
                red.append(red_copy(s, t))
                red[-1].start()

    gpair.wait_recv()
    gf_sum[...] = (gf_own[core].astype(F32) + gf_got[...].astype(F32)).astype(BF)
    spread = []
    for n in range(1, CHIPS):
        to = lax.rem(chip + n, CHIPS)
        spread.append(
            remote(gf_sum.at[to], gf_in.at[n - 1], gx_s.at[n - 1], gx_r.at[n - 1], device(y, zl, to, core))
        )
        spread[-1].start()

    red_step(2)
    red_step(3)
    red_step(4)

    total = gs_own[y].astype(F32)
    parts = []
    for half in range(2):
        part = gs_own[y, half * HALF : half * HALF + HALF].astype(F32)
        for s in range(4):
            if STREAMS[s][1] == half:
                red_copy(s, STREAMS[s][2]).wait_recv()
                part = part + gs_got[FIRST[s] + STREAMS[s][2] - 1].astype(F32)
        parts.append(part)
    total = jnp.concatenate(parts, axis=0).reshape(F, ZS, 8, K)
    for n in range(ZS):
        gz_own[n] = total[:, n].astype(BF)
    down = []
    for n in range(1, ZS):
        to = lax.rem(zl + n, ZS)
        down.append(remote(gz_own.at[to], gz_in.at[n - 1], z_s.at[n - 1], z_r.at[n - 1], device(y, to, chip, core)))
        down[-1].start()

    def put_out(value, out):
        turn[...] = value.reshape(8 * F, K)
        for s in range(8):
            out[s] = turn[pl.ds(s, F, stride=8), :].astype(BF)

    value = gf_sum[chip].astype(F32)
    for n in range(CHIPS - 1):
        spread[n].wait_recv()
        value = value + gf_in[n].astype(F32)
    put_out(value, grad_first)

    value = gz_own[zl].astype(F32)
    for n in range(ZS - 1):
        down[n].wait_recv()
        value = value + gz_in[n].astype(F32)
    put_out(value, grad_second.at[0])

    for copy in puts + [cross_hi] + along_x + ring + pair + red + [gpair] + spread + down:
        copy.wait_send()


def per_device(spectra, window_flags, pair_mask, misfit_weight, observed):
    dma = pltpu.SemaphoreType.DMA
    vmem = pltpu.VMEM
    return pl.pallas_call(
        kernel,
        out_shape=(
            jax.ShapeDtypeStruct((8, F, K), BF),
            jax.ShapeDtypeStruct((1, 8, F, K), BF),
        ),
        in_specs=[pl.BlockSpec(memory_space=pl.ANY)] * 5,
        out_specs=[pl.BlockSpec(memory_space=pltpu.VMEM)] * 2,
        scratch_shapes=[
            vmem((8, F, K), BF),
            vmem((8, K // 2), jnp.int32),
            vmem((128, 256), jnp.int32),
            vmem((F, 128, 256), BF),
            vmem((2, F, 128, 256), BF),
            vmem((8 * F, K), F32),
            vmem((F, 8, K), BF),
            vmem((CHIPS, F, 16, K), BF),
            vmem((CHIPS, F, 2, 16, K), BF),
            vmem((2, CHIPS, F, 8, K), BF),
            vmem((CHIPS, F, 8, K), BF),
            vmem((CHIPS, F, 8, K), BF),
            vmem((CHIPS - 1, F, 8, K), BF),
            vmem((YS, F, 32, K), BF),
            vmem((MESSAGES, HALF, 32, K), BF),
            vmem((ZS, F, 8, K), BF),
            vmem((ZS - 1, F, 8, K), BF),
            dma((5,)),
            dma((4,)), dma((4,)),
            dma, dma,
            dma((6,)), dma((6,)),
            dma, dma,
            dma((MESSAGES,)), dma((MESSAGES,)),
            dma, dma,
            dma((7,)), dma((7,)),
            dma((MESSAGES,)), dma((MESSAGES,)),
            dma((3,)), dma((3,)),
        ],
        compiler_params=pltpu.CompilerParams(collective_id=0, has_side_effects=True),
    )(spectra, window_flags, pair_mask, misfit_weight, observed)


def solution(mesh):
    placed = (
        P(("row", "col"), None, None),
        P(("row", "col"), None),
        P("row", "col"),
        P(None, "row", "col"),
        P(None, None, "row", "col"),
    )
    return jax.shard_map(
        per_device,
        mesh=mesh,
        in_specs=placed,
        out_specs=(P(("row", "col"), None, None), P("col", "row", None, None)),
        check_vma=False,
    )
```

```python
import jax
import jax.numpy as jnp
from jax import lax
from jax.experimental import pallas as pl
from jax.experimental.pallas import tpu as pltpu
from jax.sharding import PartitionSpec as P

MESH = pl.DeviceIdType.MESH
BF = jnp.bfloat16
F32 = jnp.float32
F = 16
K = 128
CHIPS = 8
YS = 8
ZS = 4
GROUPS = 4
G = F // GROUPS
HALF = F // 2
UNROLL = 2
WAYS = (1, -1)


def steps_of(group, way):
    return 4 if (group + way) % 2 == 0 else 3


MESSAGE = {}
for _g in range(GROUPS):
    for _w in range(2):
        for _t in range(1, steps_of(_g, _w) + 1):
            MESSAGE[_g, _w, _t] = len(MESSAGE)
MESSAGES = len(MESSAGE)


def shift_of(here, there):
    hi = lax.rem(here // 4 + there // 4, 2)
    dx = lax.rem(here - there + 8, 4)
    same = 4 - dx + 4 * (dx // 2)
    other = lax.rem(2 - dx + 8, 8)
    return hi * other + (1 - hi) * same


def chip_at(there, y):
    dy = lax.rem(y - there + 8, 8)
    hi = 1 - lax.rem(dy + 1, 8) // 4
    dx = lax.rem(hi * 2 + (1 - hi) * 4 - dy + 8, 4)
    return lax.rem(there // 4 + hi, 2) * 4 + lax.rem(there + dx, 4)


def kernel(
    spectra, flags, mask, weight, observed, out,
    spec_v, flag_v, mask_v, weight_v, obs_v, turn, mine, first, second,
    gf_own, gf_got, gf_sum, gf_in, gh_own, gh_in, gs_own, gs_got, gz_own, gz_in,
    load_sem, put_s, put_r, zs_s, zs_r, hi_s, hi_r, x_s, x_r, pair_s, pair_r, ring_s, ring_r,
    gp_s, gp_r, gx_s, gx_r, gh_s, gh_r, red_s, red_r, z_s, z_r,
):
    row = lax.axis_index("row")
    col = lax.axis_index("col")
    y, zl = row // ZS, lax.rem(row, ZS)
    chip, core = col // 2, lax.rem(col, 2)
    hi, x = chip // 4, lax.rem(chip, 4)

    def device(y, zl, chip, core):
        return (y * ZS + zl, chip * 2 + core)

    def step_y(n):
        return lax.rem(y + n + 2 * YS, YS)

    sent = []

    def remote(src, dst, send, recv, to):
        return pltpu.make_async_remote_copy(
            src_ref=src, dst_ref=dst, send_sem=send, recv_sem=recv, device_id=to, device_id_type=MESH
        )

    def send(*args):
        sent.append(remote(*args))
        sent[-1].start()

    def group(g):
        return slice(g * G, g * G + G)

    def half(n):
        return slice(n * HALF, n * HALF + HALF)

    def eight(c):
        return pl.ds(pl.multiple_of(c * 8, 8), 8)

    loads = [
        pltpu.make_async_copy(a, b, load_sem.at[n])
        for n, (a, b) in enumerate(
            ((spectra, spec_v), (flags, flag_v), (mask, mask_v), (weight, weight_v), (observed, obs_v))
        )
    ]
    loads[0].start()
    loads[1].start()

    barrier = pltpu.get_barrier_semaphore()
    partner = device(y, zl, chip, 1 - core)
    far = lax.rem(hi + 1, 2) * 4 + x
    giver = chip_at(chip, y)
    holder = zl // 2 == core
    row_chips = [device(y, zl, hi * 4 + lax.rem(x + n, 4), core) for n in range(1, 4)]
    z_line = [device(y, lax.rem(zl + n, ZS), chip, core) for n in range(1, ZS)]
    peers = [partner, device(y, zl, far, core)] + row_chips + z_line
    peers += [device(step_y(way), zl, chip, core) for way in WAYS]
    for peer in peers:
        pl.semaphore_signal(barrier, inc=1, device_id=peer, device_id_type=MESH)

    @pl.when(holder)
    def _():
        for c in range(2):
            pl.semaphore_signal(barrier, inc=1, device_id=device(chip, zl, giver, c), device_id_type=MESH)

    for load in loads[2:]:
        load.start()

    loads[0].wait()
    loads[1].wait()
    turn[...] = spec_v[...].astype(F32).reshape(8 * F, K)
    flag = flag_v[...].astype(F32)
    flag = jnp.concatenate([flag, flag], axis=1)
    pieces = [(turn[pl.ds(f, 8, stride=F), :] * flag).astype(BF) for f in range(F)]
    for f in range(F):
        mine[f] = pieces[f]

    for c in range(2):

        @pl.when(core == c)
        def _():
            for f in range(F):
                first[chip, f, 8 * c : 8 * c + 8, :] = pieces[f]

    pl.semaphore_wait(barrier, len(peers) + 1)

    to = device(lax.rem(y + shift_of(chip, y), YS), zl, y, zl // 2)
    send(mine, second.at[chip, :, lax.rem(zl, 2), eight(core), :], put_s, put_r.at[core], to)

    send(mine, first.at[chip, :, eight(core), :], hi_s, hi_r, device(y, zl, far, core))
    for n in range(3):
        send(mine, first.at[chip, :, eight(core), :], x_s.at[n], x_r.at[n], row_chips[n])

    def spread_copies(g):
        block = second.at[giver, group(g), lax.rem(zl, 2)]
        return [
            remote(block, block, zs_s.at[g * 3 + n], zs_r.at[g * 2 + lax.rem(zl, 2)], z_line[n]) for n in range(3)
        ]

    @pl.when(holder)
    def _():
        for c in range(2):
            remote(
                mine, second.at[giver, :, lax.rem(zl, 2), 8 * c : 8 * c + 8, :], put_s, put_r.at[c], partner
            ).wait_recv()
        for g in range(GROUPS):
            for copy in spread_copies(g):
                copy.start()

    def spread_arrival(g, b):
        block = second.at[giver, group(g), b]
        remote(block, block, zs_s.at[0], zs_r.at[g * 2 + b], partner).wait_recv()

    def ring_copy(g, w, t, arrival=0):
        way = WAYS[w]
        block = second.at[chip_at(chip, step_y(-way * (t - 1 + arrival))), group(g)]
        n = MESSAGE[g, w, t]
        return (block, block, ring_s.at[n], ring_r.at[n], device(step_y(way), zl, chip, core))

    def ring_step(t):
        for g in range(GROUPS):
            for w in range(2):
                if t <= steps_of(g, w):
                    remote(*ring_copy(g, w, t - 1, 1)).wait_recv()
                    send(*ring_copy(g, w, t))

    for g in range(GROUPS):

        @pl.when(holder)
        def _():
            spread_arrival(g, 1 - lax.rem(zl, 2))

        @pl.when(jnp.logical_not(holder))
        def _():
            spread_arrival(g, 0)
            spread_arrival(g, 1)

        for w in range(2):
            send(*ring_copy(g, w, 1))

    block = first.at[far, :, eight(core), :]
    remote(mine, block, hi_s, hi_r, partner).wait_recv()
    for n in range(3):
        send(block, block, x_s.at[n + 3], x_r.at[n + 3], row_chips[n])

    def to_partner(n):
        z_hi = hi if n == 0 else lax.rem(hi + 1, 2)
        for m in range(3):
            from_chip = z_hi * 4 + lax.rem(x - m - 1 + 4, 4)
            remote(
                mine, first.at[from_chip, :, eight(core), :], x_s.at[0], x_r.at[n * 3 + m], partner
            ).wait_recv()
        block = first.at[pl.ds(z_hi * 4, 4), :, eight(core), :]
        send(block, block, pair_s.at[n], pair_r.at[n], partner)

    ring_step(2)
    to_partner(0)
    ring_step(3)
    to_partner(1)
    ring_step(4)
    for n in range(2):
        z_hi = hi if n == 0 else lax.rem(hi + 1, 2)
        block = first.at[pl.ds(z_hi * 4, 4), :, eight(1 - core), :]
        remote(block, block, pair_s.at[n], pair_r.at[n], partner).wait_recv()
    for load in loads[2:]:
        load.wait()

    lane = lax.broadcasted_iota(jnp.int32, (1, K), 1)
    sign = jnp.where(lane < K // 2, 1.0, -1.0).astype(F32)

    def one_frequency(f):
        v = first[:, f].reshape(128, K)
        turned = (pltpu.roll(v.astype(F32), K // 2, 1) * sign).astype(BF)
        rows = jnp.concatenate([v, turned], axis=0)
        cols = jnp.concatenate([second[:, f, b].reshape(128, K) for b in range(2)], axis=0)
        cross = lax.dot_general(rows, cols, (((1,), (1,)), ((), ())), preferred_element_type=F32)
        scale = mask_v[...].astype(F32) * weight_v[f].astype(F32)
        residual = jnp.concatenate(
            [(scale * (cross[128 * c : 128 * c + 128] - obs_v[c, f].astype(F32))).astype(BF) for c in range(2)], axis=0
        )
        prod = jnp.dot(residual, cols, preferred_element_type=F32)
        gf = prod[:128] - pltpu.roll(prod[128:], K // 2, 1) * sign
        gf = gf.reshape(CHIPS, 2, 8, K)
        for c in range(2):
            gf_own[c, :, f] = gf[:, c].astype(BF)
        gs = lax.dot_general(residual, rows, (((0,), (0,)), ((), ())), preferred_element_type=F32)
        gs_own[:, f] = gs.reshape(YS, 32, K).astype(BF)

    def compute(g):
        for w in range(2):
            remote(*ring_copy(g, w, steps_of(g, w), 1)).wait_recv()

        def pair_of(n, carry):
            for m in range(UNROLL):
                one_frequency(g * G + n * UNROLL + m)
            return carry

        lax.fori_loop(0, G // UNROLL, pair_of, 0)

    def red_copy(g, w, t):
        way = WAYS[w]
        n = MESSAGE[g, w, t]
        src = gs_own.at[step_y(way * (steps_of(g, w) - t + 1)), group(g)]
        return (src, gs_got.at[n], red_s.at[n], red_r.at[n], device(step_y(way), zl, chip, core))

    def reduce(g, t):
        for w in range(2):
            steps = steps_of(g, w)
            if t > steps:
                continue
            if t > 1:
                remote(*red_copy(g, w, t - 1)).wait_recv()
                acc = gs_own.at[step_y(WAYS[w] * (steps - t + 1)), group(g)]
                acc[...] = (acc[...].astype(F32) + gs_got[MESSAGE[g, w, t - 1]].astype(F32)).astype(BF)
            send(*red_copy(g, w, t))

    def reduced(g):
        total = gs_own[y, group(g)].astype(F32)
        for w in range(2):
            steps = steps_of(g, w)
            remote(*red_copy(g, w, steps)).wait_recv()
            total = total + gs_got[MESSAGE[g, w, steps]].astype(F32)
        total = total.reshape(G, ZS, 8, K)
        for n in range(ZS):
            gz_own[n, group(g)] = total[:, n].astype(BF)
        for n in range(3):
            send(*z_copy(g, n))

    def z_copy(g, n):
        to = lax.rem(zl + n + 1, ZS)
        m = g * 3 + n
        return (gz_own.at[to, group(g)], gz_in.at[n, group(g)], z_s.at[m], z_r.at[m], z_line[n])

    def gf_pair(n):
        return (gf_own.at[1 - core, :, half(n)], gf_got.at[:, half(n)], gp_s.at[n], gp_r.at[n], partner)

    def gf_x(n, m):
        to = lax.rem(x + m + 1, 4)
        return (gf_sum.at[:, to, half(n)], gf_in.at[m, :, half(n)], gx_s.at[n * 3 + m], gx_r.at[n * 3 + m], row_chips[m])

    def gf_hi(n):
        return (gh_own.at[1 - hi, half(n)], gh_in.at[half(n)], gh_s.at[n], gh_r.at[n], device(y, zl, far, core))

    def gf_along_x(n):
        remote(*gf_pair(n)).wait_recv()
        value = gf_own[core, :, half(n)].astype(F32) + gf_got[:, half(n)].astype(F32)
        gf_sum[:, :, half(n)] = value.astype(BF).reshape(2, 4, HALF, 8, K)
        for m in range(3):
            send(*gf_x(n, m))

    def gf_across(n):
        value = gf_sum[:, x, half(n)].astype(F32)
        for m in range(3):
            remote(*gf_x(n, m)).wait_recv()
            value = value + gf_in[m, :, half(n)].astype(F32)
        gh_own[:, half(n)] = value.astype(BF)
        send(*gf_hi(n))

    compute(0)
    reduce(0, 1)
    compute(1)
    reduce(1, 1)
    send(*gf_pair(0))
    compute(2)
    reduce(2, 1)
    reduce(0, 2)
    gf_along_x(0)
    compute(3)
    reduce(3, 1)
    send(*gf_pair(1))
    reduce(1, 2)
    reduce(2, 2)
    reduce(0, 3)
    gf_along_x(1)
    reduce(3, 2)
    reduce(1, 3)
    gf_across(0)
    reduce(2, 3)
    reduce(0, 4)
    reduce(3, 3)
    reduce(1, 4)
    gf_across(1)
    reduce(2, 4)
    reduce(3, 4)
    for g in range(GROUPS):
        reduced(g)

    def put_out(value, out):
        turn[...] = value.reshape(8 * F, K)
        for s in range(8):
            out[s] = turn[pl.ds(s, F, stride=8), :].astype(BF)

    for n in range(2):
        remote(*gf_hi(n)).wait_recv()
    put_out(gh_own[hi].astype(F32) + gh_in[...].astype(F32), out.at[0])

    value = gz_own[zl].astype(F32)
    for n in range(3):
        for g in range(GROUPS):
            remote(*z_copy(g, n)).wait_recv()
        value = value + gz_in[n].astype(F32)
    put_out(value, out.at[1])

    for copy in sent:
        copy.wait_send()

    @pl.when(holder)
    def _():
        for g in range(GROUPS):
            for copy in spread_copies(g):
                copy.wait_send()


def finish(both, grad_first, grad_second):
    grad_first[...] = both[0]
    grad_second[0] = both[1]


def per_device(spectra, window_flags, pair_mask, misfit_weight, observed):
    dma = pltpu.SemaphoreType.DMA
    vmem = pltpu.VMEM
    both = pl.pallas_call(
        kernel,
        out_shape=jax.ShapeDtypeStruct((2, 8, F, K), BF),
        in_specs=[pl.BlockSpec(memory_space=pl.ANY)] * 5,
        out_specs=pl.BlockSpec(memory_space=pltpu.VMEM),
        scratch_shapes=[
            vmem((8, F, K), BF),
            vmem((8, K // 2), jnp.int32),
            vmem((128, 256), jnp.int32),
            vmem((F, 128, 256), BF),
            vmem((2, F, 128, 256), BF),
            vmem((8 * F, K), F32),
            vmem((F, 8, K), BF),
            vmem((CHIPS, F, 16, K), BF),
            vmem((CHIPS, F, 2, 16, K), BF),
            vmem((2, CHIPS, F, 8, K), BF),
            vmem((CHIPS, F, 8, K), BF),
            vmem((2, 4, F, 8, K), BF),
            vmem((3, 2, F, 8, K), BF),
            vmem((2, F, 8, K), BF),
            vmem((F, 8, K), BF),
            vmem((YS, F, 32, K), BF),
            vmem((MESSAGES, G, 32, K), BF),
            vmem((ZS, F, 8, K), BF),
            vmem((ZS - 1, F, 8, K), BF),
            dma((5,)),
            dma, dma((2,)),
            dma((3 * GROUPS,)), dma((2 * GROUPS,)),
            dma, dma,
            dma((6,)), dma((6,)),
            dma((2,)), dma((2,)),
            dma((MESSAGES,)), dma((MESSAGES,)),
            dma((2,)), dma((2,)),
            dma((6,)), dma((6,)),
            dma((2,)), dma((2,)),
            dma((MESSAGES,)), dma((MESSAGES,)),
            dma((3 * GROUPS,)), dma((3 * GROUPS,)),
        ],
        compiler_params=pltpu.CompilerParams(collective_id=0, has_side_effects=True),
    )(spectra, window_flags, pair_mask, misfit_weight, observed)
    return pl.pallas_call(
        finish,
        out_shape=(
            jax.ShapeDtypeStruct((8, F, K), BF),
            jax.ShapeDtypeStruct((1, 8, F, K), BF),
        ),
        in_specs=[pl.BlockSpec(memory_space=pltpu.VMEM)],
        out_specs=[pl.BlockSpec(memory_space=pltpu.VMEM)] * 2,
    )(both)


def solution(mesh):
    placed = (
        P(("row", "col"), None, None),
        P(("row", "col"), None),
        P("row", "col"),
        P(None, "row", "col"),
        P(None, None, "row", "col"),
    )
    return jax.shard_map(
        per_device,
        mesh=mesh,
        in_specs=placed,
        out_specs=(P(("row", "col"), None, None), P("col", "row", None, None)),
        check_vma=False,
    )
```

```python
import functools

import jax
import jax.numpy as jnp
from jax import lax
from jax.experimental import pallas as pl
from jax.experimental.pallas import tpu as pltpu
from jax.sharding import PartitionSpec as P

MESH = pl.DeviceIdType.MESH
BF = jnp.bfloat16
F32 = jnp.float32
F = 16
K = 128
CHIPS = 8
YS = 8
ZS = 4
GROUPS = 4
G = F // GROUPS
HALF = F // 2
UNROLL = 16
WAYS = (1, -1)


def steps_of(group, way):
    return 4 if (group + way) % 2 == 0 else 3


MESSAGE = {}
for _g in range(GROUPS):
    for _w in range(2):
        for _t in range(1, steps_of(_g, _w) + 1):
            MESSAGE[_g, _w, _t] = len(MESSAGE)
MESSAGES = len(MESSAGE)


def landing(zl, chip, other):
    mirrored = lax.rem(chip // 4 + other // 4, 2)
    return mirrored * (ZS - 1 - zl) + (1 - mirrored) * zl


def kernel(
    spectra, flags, mask, weight, observed, out,
    spec_v, flag_v, mask_v, weight_v, obs_v, turn, mine, first, second,
    scale_t, obs_t, rows_v, res_t,
    gf_own, gf_got, gf_sum, gf_in, gh_own, gh_in, gs_own, gs_got, gz_own, gz_in,
    load_sem, put_s, put_r, zs_s, zs_r, hi_s, hi_r, x_s, x_r, pair_s, pair_r, ring_s, ring_r,
    gp_s, gp_r, gx_s, gx_r, gh_s, gh_r, red_s, red_r, z_s, z_r,
):
    row = lax.axis_index("row")
    col = lax.axis_index("col")
    y, zl = row // ZS, lax.rem(row, ZS)
    chip, core = col // 2, lax.rem(col, 2)
    hi, x = chip // 4, lax.rem(chip, 4)

    def device(y, zl, chip, core):
        return (y * ZS + zl, chip * 2 + core)

    def step_y(n):
        return lax.rem(y + n + 2 * YS, YS)

    sent = []

    def remote(src, dst, send, recv, to):
        return pltpu.make_async_remote_copy(
            src_ref=src, dst_ref=dst, send_sem=send, recv_sem=recv, device_id=to, device_id_type=MESH
        )

    def send(*args):
        sent.append(remote(*args))
        sent[-1].start()

    def group(g):
        return slice(g * G, g * G + G)

    def half(n):
        return slice(n * HALF, n * HALF + HALF)

    def eight(c):
        return pl.ds(pl.multiple_of(c * 8, 8), 8)

    loads = [
        pltpu.make_async_copy(a, b, load_sem.at[n])
        for n, (a, b) in enumerate(
            ((spectra, spec_v), (flags, flag_v), (mask, mask_v), (weight, weight_v), (observed, obs_v))
        )
    ]
    loads[0].start()
    loads[1].start()

    barrier = pltpu.get_barrier_semaphore()
    partner = device(y, zl, chip, 1 - core)
    far = lax.rem(hi + 1, 2) * 4 + x
    own = lax.rem(y, 4)
    held = landing(zl, chip, 2 * own)
    holder = held // 2 == core
    stays = jnp.logical_and(jnp.logical_and(chip == y, chip // 2 == own), zl // 2 == core)
    my_piece = lax.rem(chip, 2) * 2 + core

    def unless_stays(is_it, body):
        pl.when(jnp.logical_not(jnp.logical_and(stays, is_it)))(body)

    block_chips = [lax.rem(chip + n, CHIPS) for n in (4, 5, 3, 6, 2, 7, 1)]
    row_chips = [device(y, zl, hi * 4 + lax.rem(x + n, 4), core) for n in range(1, 4)]
    z_line = [device(y, lax.rem(zl + n, ZS), chip, core) for n in range(1, ZS)]
    peers = [partner] + [device(y, zl, to, core) for to in block_chips] + z_line
    peers += [device(step_y(way), zl, chip, core) for way in WAYS]
    for peer in peers:
        pl.semaphore_signal(barrier, inc=1, device_id=peer, device_id_type=MESH)

    @pl.when(holder)
    def _():
        for n in range(4):

            @functools.partial(unless_stays, my_piece == n)
            def _():
                giver = device(chip, held, 2 * own + n // 2, n % 2)
                pl.semaphore_signal(barrier, inc=1, device_id=giver, device_id_type=MESH)

    for load in loads[2:]:
        load.start()

    loads[0].wait()
    loads[1].wait()
    turn[...] = spec_v[...].astype(F32).reshape(8 * F, K)
    flag = flag_v[...].astype(F32)
    flag = jnp.concatenate([flag, flag], axis=1)
    pieces = [(turn[pl.ds(f, 8, stride=F), :] * flag).astype(BF) for f in range(F)]
    for f in range(F):
        mine[f] = pieces[f]

    for c in range(2):

        @pl.when(core == c)
        def _():
            for f in range(F):
                first[chip, f, 8 * c : 8 * c + 8, :] = pieces[f]

            @pl.when(stays)
            def _():
                for f in range(F):
                    second[chip, f, lax.rem(zl, 2), 8 * c : 8 * c + 8, :] = pieces[f]

    @pl.when(stays)
    def _():
        pl.semaphore_wait(barrier, len(peers) + 1)

    @functools.partial(unless_stays, True)
    def _():
        pl.semaphore_wait(barrier, len(peers) + 2)


    def put(g, n):
        to = device(chip // 2 + 4 * n, landing(zl, chip, y), y, zl // 2)
        dst = second.at[chip, group(g), lax.rem(zl, 2), eight(core), :]
        return remote(mine.at[group(g)], dst, put_s.at[g * 2 + n], put_r.at[g * 4 + my_piece], to)

    for n in range(2):

        @functools.partial(unless_stays, y // 4 == n)
        def _():
            for g in range(GROUPS):
                put(g, n).start()

    send(mine, first.at[chip, :, eight(core), :], hi_s, hi_r, device(y, zl, far, core))
    for n in range(3):
        send(mine, first.at[chip, :, eight(core), :], x_s.at[n], x_r.at[n], row_chips[n])

    for load in loads[2:]:
        load.wait()

    def over(first_f, last_f, body):
        def several(n, carry):
            for m in range(min(UNROLL, last_f - first_f)):
                body(first_f + n * min(UNROLL, last_f - first_f) + m)
            return carry

        lax.fori_loop(0, (last_f - first_f) // min(UNROLL, last_f - first_f), several, 0)

    def prepare(f):
        scale = mask_v[...].astype(F32).astype(BF) * weight_v[f]
        scale_t[f] = scale.T.reshape(2, 4, 32, 128)
        for c in range(2):
            obs_t[f, c] = obs_v[c, f].T.reshape(2, 4, 32, 128)

    over(0, HALF, prepare)

    def spread_copies(g):
        block = second.at[pl.ds(2 * own, 2), group(g), lax.rem(held, 2)]
        return [
            remote(block, block, zs_s.at[g * 3 + n], zs_r.at[g * 2 + lax.rem(held, 2)], z_line[n]) for n in range(3)
        ]

    def spread(g):
        @pl.when(holder)
        def _():
            for n in range(4):

                @functools.partial(unless_stays, my_piece == n)
                def _():
                    c = n % 2
                    block = second.at[2 * own + n // 2, group(g), lax.rem(held, 2), 8 * c : 8 * c + 8, :]
                    remote(mine.at[group(g)], block, put_s.at[0], put_r.at[g * 4 + n], partner).wait_recv()

            for copy in spread_copies(g):
                copy.start()

    spread(0)
    spread(1)

    block = first.at[far, :, eight(core), :]
    remote(mine, block, hi_s, hi_r, partner).wait_recv()
    for n in range(3):
        send(block, block, x_s.at[n + 3], x_r.at[n + 3], row_chips[n])

    def to_partner(n):
        z_hi = hi if n == 0 else lax.rem(hi + 1, 2)
        for m in range(3):
            from_chip = z_hi * 4 + lax.rem(x - m - 1 + 4, 4)
            remote(
                mine, first.at[from_chip, :, eight(core), :], x_s.at[0], x_r.at[n * 3 + m], partner
            ).wait_recv()
        block = first.at[pl.ds(z_hi * 4, 4), :, eight(core), :]
        send(block, block, pair_s.at[n], pair_r.at[n], partner)

    over(HALF, F, prepare)
    to_partner(0)

    def spread_arrival(g, b):
        block = second.at[pl.ds(2 * own, 2), group(g), b]
        remote(block, block, zs_s.at[0], zs_r.at[g * 2 + b], partner).wait_recv()

    def ring_copy(g, w, t, arrival=0):
        way = WAYS[w]
        m = lax.rem(step_y(-way * (t - 1 + arrival)), 4)
        block = second.at[pl.ds(2 * m, 2), group(g)] if t == 1 else second.at[2 * m + w, group(g)]
        n = (g * 2 + w) * 2 + t - 1
        return (block, block, ring_s.at[n], ring_r.at[n], device(step_y(way), zl, chip, core))

    def ring_second():
        for g in range(GROUPS):
            for w in range(2):
                remote(*ring_copy(g, w, 1, 1)).wait_recv()
                send(*ring_copy(g, w, 2))

    def ring_end():
        for g in range(GROUPS):
            for w in range(2):
                remote(*ring_copy(g, w, 2, 1)).wait_recv()

    def ring_first(g):
        @pl.when(holder)
        def _():
            spread_arrival(g, 1 - lax.rem(held, 2))

        @pl.when(jnp.logical_not(holder))
        def _():
            spread_arrival(g, 0)
            spread_arrival(g, 1)

        for w in range(2):
            send(*ring_copy(g, w, 1))

    spread(2)
    ring_first(0)
    spread(3)
    for g in range(1, GROUPS):
        ring_first(g)

    lane = lax.broadcasted_iota(jnp.int32, (1, K), 1)
    sign = jnp.where(lane < K // 2, 1.0, -1.0).astype(F32)

    def build_rows(f):
        v = first[:, f].reshape(128, K)
        rows_v[f, 0] = v
        rows_v[f, 1] = (pltpu.roll(v.astype(F32), K // 2, 1) * sign).astype(BF)

    def compute(pairs):
        def one(f):
            rows = rows_v[f].reshape(256, K)
            cols = jnp.concatenate(
                [second[pl.ds(2 * m, 2), f, b].reshape(32, K) for m in pairs for b in range(2)], axis=0
            )
            twice = 1 if len(pairs) > 1 else 2
            cols = jnp.concatenate([cols] * twice, axis=0)
            cross = lax.dot_general(cols, rows, (((1,), (1,)), ((), ())), preferred_element_type=F32)
            blocks = []
            for n, m in enumerate(pairs):
                for b in range(2):
                    at = (2 * n + b) * 32
                    scale = scale_t[f, b, m].astype(F32)
                    block = [
                        (scale * (cross[at : at + 32, 128 * c : 128 * c + 128] - obs_t[f, c, b, m].astype(F32))).astype(BF)
                        for c in range(2)
                    ]
                    blocks.append(jnp.concatenate(block, axis=1))
                    res_t[f, b, m] = blocks[-1]
            gs = jnp.dot(jnp.concatenate(blocks * twice, axis=0), rows, preferred_element_type=F32)
            for n, m in enumerate(pairs):
                for b in range(2):
                    at = (2 * n + b) * 32
                    gs_own[4 * b + m, f] = gs[at : at + 32].astype(BF)

        over(0, F, one)

    def first_gradient(f):
        residual = res_t[f].reshape(256, 256)
        cols = jnp.concatenate([second[:, f, b].reshape(128, K) for b in range(2)], axis=0)
        prod = lax.dot_general(residual, cols, (((0,), (0,)), ((), ())), preferred_element_type=F32)
        gf = prod[:128] - pltpu.roll(prod[128:], K // 2, 1) * sign
        gf = gf.reshape(CHIPS, 2, 8, K)
        for c in range(2):
            gf_own[c, :, f] = gf[:, c].astype(BF)

    def red_copy(g, w, t):
        way = WAYS[w]
        n = MESSAGE[g, w, t]
        src = gs_own.at[step_y(way * (steps_of(g, w) - t + 1)), group(g)]
        return (src, gs_got.at[n], red_s.at[n], red_r.at[n], device(step_y(way), zl, chip, core))

    def reduce(distance, start=0, stop=GROUPS):
        for g in range(start, stop):
            for w in range(2):
                t = steps_of(g, w) - distance + 1
                if t < 1:
                    continue
                if t > 1:
                    remote(*red_copy(g, w, t - 1)).wait_recv()
                    acc = gs_own.at[step_y(WAYS[w] * distance), group(g)]
                    acc[...] = (acc[...].astype(F32) + gs_got[MESSAGE[g, w, t - 1]].astype(F32)).astype(BF)
                send(*red_copy(g, w, t))

    def reduced(g):
        total = gs_own[y, group(g)].astype(F32)
        for w in range(2):
            steps = steps_of(g, w)
            remote(*red_copy(g, w, steps)).wait_recv()
            total = total + gs_got[MESSAGE[g, w, steps]].astype(F32)
        total = total.reshape(G, ZS, 8, K)
        for n in range(ZS):
            gz_own[n, group(g)] = total[:, n].astype(BF)
        for n in range(3):
            send(*z_copy(g, n))

    def z_copy(g, n):
        to = lax.rem(zl + n + 1, ZS)
        m = g * 3 + n
        return (gz_own.at[to, group(g)], gz_in.at[n, group(g)], z_s.at[m], z_r.at[m], z_line[n])

    def gf_pair(n):
        return (gf_own.at[1 - core, :, half(n)], gf_got.at[:, half(n)], gp_s.at[n], gp_r.at[n], partner)

    def gf_x(n, m):
        to = lax.rem(x + m + 1, 4)
        return (gf_sum.at[:, to, half(n)], gf_in.at[m, :, half(n)], gx_s.at[n * 3 + m], gx_r.at[n * 3 + m], row_chips[m])

    def gf_hi(n):
        return (gh_own.at[1 - hi, half(n)], gh_in.at[half(n)], gh_s.at[n], gh_r.at[n], device(y, zl, far, core))

    def gf_along_x(n):
        remote(*gf_pair(n)).wait_recv()
        value = gf_own[core, :, half(n)].astype(F32) + gf_got[:, half(n)].astype(F32)
        gf_sum[:, :, half(n)] = value.astype(BF).reshape(2, 4, HALF, 8, K)
        for m in range(3):
            send(*gf_x(n, m))

    def gf_across(n):
        value = gf_sum[:, x, half(n)].astype(F32)
        for m in range(3):
            remote(*gf_x(n, m)).wait_recv()
            value = value + gf_in[m, :, half(n)].astype(F32)
        gh_own[:, half(n)] = value.astype(BF)
        send(*gf_hi(n))

    to_partner(1)
    for n in range(2):
        z_hi = hi if n == 0 else lax.rem(hi + 1, 2)
        block = first.at[pl.ds(z_hi * 4, 4), :, eight(1 - core), :]
        remote(block, block, pair_s.at[n], pair_r.at[n], partner).wait_recv()
    over(0, F, build_rows)
    compute([own])
    reduce(4)
    ring_second()
    compute([lax.rem(y + 1, 4), lax.rem(y + 3, 4)])
    reduce(3)
    ring_end()
    compute([lax.rem(y + 2, 4)])
    over(0, HALF, first_gradient)
    send(*gf_pair(0))
    reduce(2)
    over(HALF, F, first_gradient)
    send(*gf_pair(1))
    gf_along_x(0)
    reduce(1, 0, 2)
    gf_along_x(1)
    reduce(1, 2, 4)
    gf_across(0)
    reduced(0)
    reduced(1)
    gf_across(1)
    reduced(2)
    reduced(3)

    def put_out(value, out):
        turn[...] = value.reshape(8 * F, K)
        for s in range(8):
            out[s] = turn[pl.ds(s, F, stride=8), :].astype(BF)

    for n in range(2):
        remote(*gf_hi(n)).wait_recv()
    put_out(gh_own[hi].astype(F32) + gh_in[...].astype(F32), out.at[0])

    value = gz_own[zl].astype(F32)
    for n in range(3):
        for g in range(GROUPS):
            remote(*z_copy(g, n)).wait_recv()
        value = value + gz_in[n].astype(F32)
    put_out(value, out.at[1])

    for copy in sent:
        copy.wait_send()
    for n in range(2):

        @functools.partial(unless_stays, y // 4 == n)
        def _():
            for g in range(GROUPS):
                put(g, n).wait_send()


    @pl.when(holder)
    def _():
        for g in range(GROUPS):
            for copy in spread_copies(g):
                copy.wait_send()


def finish(both, grad_first, grad_second):
    grad_first[...] = both[0]
    grad_second[0] = both[1]


def per_device(spectra, window_flags, pair_mask, misfit_weight, observed):
    dma = pltpu.SemaphoreType.DMA
    vmem = pltpu.VMEM
    both = pl.pallas_call(
        kernel,
        out_shape=jax.ShapeDtypeStruct((2, 8, F, K), BF),
        in_specs=[pl.BlockSpec(memory_space=pl.ANY)] * 5,
        out_specs=pl.BlockSpec(memory_space=pltpu.VMEM),
        scratch_shapes=[
            vmem((8, F, K), BF),
            vmem((8, K // 2), jnp.int32),
            vmem((128, 256), jnp.int32),
            vmem((F, 128, 256), BF),
            vmem((2, F, 128, 256), BF),
            vmem((8 * F, K), F32),
            vmem((F, 8, K), BF),
            vmem((CHIPS, F, 16, K), BF),
            vmem((CHIPS, F, 2, 16, K), BF),
            vmem((F, 2, 4, 32, 128), BF),
            vmem((F, 2, 2, 4, 32, 128), BF),
            vmem((F, 2, 128, K), BF),
            vmem((F, 2, 4, 32, 256), BF),
            vmem((2, CHIPS, F, 8, K), BF),
            vmem((CHIPS, F, 8, K), BF),
            vmem((2, 4, F, 8, K), BF),
            vmem((3, 2, F, 8, K), BF),
            vmem((2, F, 8, K), BF),
            vmem((F, 8, K), BF),
            vmem((YS, F, 32, K), BF),
            vmem((MESSAGES, G, 32, K), BF),
            vmem((ZS, F, 8, K), BF),
            vmem((ZS - 1, F, 8, K), BF),
            dma((5,)),
            dma((2 * GROUPS,)), dma((4 * GROUPS,)),
            dma((3 * GROUPS,)), dma((2 * GROUPS,)),
            dma, dma,
            dma((6,)), dma((6,)),
            dma((2,)), dma((2,)),
            dma((4 * GROUPS,)), dma((4 * GROUPS,)),
            dma((2,)), dma((2,)),
            dma((6,)), dma((6,)),
            dma((2,)), dma((2,)),
            dma((MESSAGES,)), dma((MESSAGES,)),
            dma((3 * GROUPS,)), dma((3 * GROUPS,)),
        ],
        compiler_params=pltpu.CompilerParams(collective_id=0, has_side_effects=True),
    )(spectra, window_flags, pair_mask, misfit_weight, observed)
    return pl.pallas_call(
        finish,
        out_shape=(
            jax.ShapeDtypeStruct((8, F, K), BF),
            jax.ShapeDtypeStruct((1, 8, F, K), BF),
        ),
        in_specs=[pl.BlockSpec(memory_space=pltpu.VMEM)],
        out_specs=[pl.BlockSpec(memory_space=pltpu.VMEM)] * 2,
    )(both)


def solution(mesh):
    placed = (
        P(("row", "col"), None, None),
        P(("row", "col"), None),
        P("row", "col"),
        P(None, "row", "col"),
        P(None, None, "row", "col"),
    )
    return jax.shard_map(
        per_device,
        mesh=mesh,
        in_specs=placed,
        out_specs=(P(("row", "col"), None, None), P("col", "row", None, None)),
        check_vma=False,
    )
```

```python
import functools

import jax
import jax.numpy as jnp
from jax import lax
from jax.experimental import pallas as pl
from jax.experimental.pallas import tpu as pltpu
from jax.sharding import PartitionSpec as P

MESH = pl.DeviceIdType.MESH
BF = jnp.bfloat16
F32 = jnp.float32
F = 16
K = 128
CHIPS = 8
YS = 8
ZS = 4
GROUPS = 2
G = F // GROUPS
HALF = F // 2
UNROLL = 16
WAYS = (1, -1)


def steps_of(group, way):
    return 4 if (group + way) % 2 == 0 else 3


MESSAGE = {}
for _g in range(GROUPS):
    for _w in range(2):
        for _t in range(1, steps_of(_g, _w) + 1):
            MESSAGE[_g, _w, _t] = len(MESSAGE)
MESSAGES = len(MESSAGE)


def landing(zl, chip, other):
    mirrored = lax.rem(chip // 4 + other // 4, 2)
    return mirrored * (ZS - 1 - zl) + (1 - mirrored) * zl


def kernel(
    spectra, flags, mask, weight, observed, out,
    spec_v, flag_v, mask_v, weight_v, obs_v, turn, mine, first, second,
    scale_t, obs_t, rows_v, res_t,
    gf_own, gf_got, gf_sum, gf_in, gh_own, gh_in, gs_own, gs_got, gz_own, gz_in,
    load_sem, put_s, put_r, zs_s, zs_r, hi_s, hi_r, x_s, x_r, pair_s, pair_r, ring_s, ring_r,
    gp_s, gp_r, gx_s, gx_r, gh_s, gh_r, red_s, red_r, z_s, z_r,
):
    row = lax.axis_index("row")
    col = lax.axis_index("col")
    y, zl = row // ZS, lax.rem(row, ZS)
    chip, core = col // 2, lax.rem(col, 2)
    hi, x = chip // 4, lax.rem(chip, 4)

    def device(y, zl, chip, core):
        return (y * ZS + zl, chip * 2 + core)

    def step_y(n):
        return lax.rem(y + n + 2 * YS, YS)

    sent = []

    def remote(src, dst, send, recv, to):
        return pltpu.make_async_remote_copy(
            src_ref=src, dst_ref=dst, send_sem=send, recv_sem=recv, device_id=to, device_id_type=MESH
        )

    def send(*args):
        sent.append(remote(*args))
        sent[-1].start()

    def group(g):
        return slice(g * G, g * G + G)

    def half(n):
        return slice(n * HALF, n * HALF + HALF)

    def eight(c):
        return pl.ds(pl.multiple_of(c * 8, 8), 8)

    loads = [
        pltpu.make_async_copy(a, b, load_sem.at[n])
        for n, (a, b) in enumerate(
            ((spectra, spec_v), (flags, flag_v), (mask, mask_v), (weight, weight_v), (observed, obs_v))
        )
    ]
    loads[0].start()
    loads[1].start()

    barrier = pltpu.get_barrier_semaphore()
    partner = device(y, zl, chip, 1 - core)
    far = lax.rem(hi + 1, 2) * 4 + x
    own = lax.rem(y, 4)
    held = landing(zl, chip, 2 * own)
    holder = held // 2 == core
    stays = jnp.logical_and(jnp.logical_and(chip == y, chip // 2 == own), zl // 2 == core)
    my_piece = lax.rem(chip, 2) * 2 + core

    def unless_stays(is_it, body):
        pl.when(jnp.logical_not(jnp.logical_and(stays, is_it)))(body)

    block_chips = [lax.rem(chip + n, CHIPS) for n in (4, 5, 3, 6, 2, 7, 1)]
    row_chips = [device(y, zl, hi * 4 + lax.rem(x + n, 4), core) for n in range(1, 4)]
    z_line = [device(y, lax.rem(zl + n, ZS), chip, core) for n in range(1, ZS)]
    peers = [partner] + [device(y, zl, to, core) for to in block_chips] + z_line
    peers += [device(step_y(way), zl, chip, core) for way in WAYS]
    for peer in peers:
        pl.semaphore_signal(barrier, inc=1, device_id=peer, device_id_type=MESH)

    @pl.when(holder)
    def _():
        for n in range(4):

            @functools.partial(unless_stays, my_piece == n)
            def _():
                giver = device(chip, held, 2 * own + n // 2, n % 2)
                pl.semaphore_signal(barrier, inc=1, device_id=giver, device_id_type=MESH)

    for load in loads[2:]:
        load.start()

    loads[0].wait()
    loads[1].wait()
    turn[...] = spec_v[...].astype(F32).reshape(8 * F, K)
    flag = flag_v[...].astype(F32)
    flag = jnp.concatenate([flag, flag], axis=1)
    pieces = [(turn[pl.ds(f, 8, stride=F), :] * flag).astype(BF) for f in range(F)]
    for f in range(F):
        mine[f] = pieces[f]

    for c in range(2):

        @pl.when(core == c)
        def _():
            for f in range(F):
                first[chip, f, 8 * c : 8 * c + 8, :] = pieces[f]

            @pl.when(stays)
            def _():
                for f in range(F):
                    second[chip, f, lax.rem(zl, 2), 8 * c : 8 * c + 8, :] = pieces[f]

    @pl.when(stays)
    def _():
        pl.semaphore_wait(barrier, len(peers) + 1)

    @functools.partial(unless_stays, True)
    def _():
        pl.semaphore_wait(barrier, len(peers) + 2)


    def put(g, n):
        to = device(chip // 2 + 4 * n, landing(zl, chip, y), y, zl // 2)
        dst = second.at[chip, group(g), lax.rem(zl, 2), eight(core), :]
        return remote(mine.at[group(g)], dst, put_s.at[g * 2 + n], put_r.at[g * 4 + my_piece], to)

    for n in range(2):

        @functools.partial(unless_stays, y // 4 == n)
        def _():
            for g in range(GROUPS):
                put(g, n).start()

    send(mine, first.at[chip, :, eight(core), :], hi_s, hi_r, device(y, zl, far, core))
    for n in range(3):
        send(mine, first.at[chip, :, eight(core), :], x_s.at[n], x_r.at[n], row_chips[n])

    for load in loads[2:]:
        load.wait()

    def over(first_f, last_f, body):
        def several(n, carry):
            for m in range(min(UNROLL, last_f - first_f)):
                body(first_f + n * min(UNROLL, last_f - first_f) + m)
            return carry

        lax.fori_loop(0, (last_f - first_f) // min(UNROLL, last_f - first_f), several, 0)

    def prepare(f):
        scale = mask_v[...].astype(F32).astype(BF) * weight_v[f]
        scale_t[f] = scale.T.reshape(2, 4, 32, 128)
        for c in range(2):
            obs_t[f, c] = obs_v[c, f].T.reshape(2, 4, 32, 128)

    over(0, F, prepare)

    def spread_copies(g):
        block = second.at[pl.ds(2 * own, 2), group(g), lax.rem(held, 2)]
        return [
            remote(block, block, zs_s.at[g * 3 + n], zs_r.at[g * 2 + lax.rem(held, 2)], z_line[n]) for n in range(3)
        ]

    def spread(g):
        @pl.when(holder)
        def _():
            for n in range(4):

                @functools.partial(unless_stays, my_piece == n)
                def _():
                    c = n % 2
                    block = second.at[2 * own + n // 2, group(g), lax.rem(held, 2), 8 * c : 8 * c + 8, :]
                    remote(mine.at[group(g)], block, put_s.at[0], put_r.at[g * 4 + n], partner).wait_recv()

            for copy in spread_copies(g):
                copy.start()


    def to_partner(n):
        z_hi = hi if n == 0 else lax.rem(hi + 1, 2)
        for m in range(3):
            from_chip = z_hi * 4 + lax.rem(x - m - 1 + 4, 4)
            remote(
                mine, first.at[from_chip, :, eight(core), :], x_s.at[0], x_r.at[n * 3 + m], partner
            ).wait_recv()
        block = first.at[pl.ds(z_hi * 4, 4), :, eight(core), :]
        send(block, block, pair_s.at[n], pair_r.at[n], partner)


    def spread_arrival(g, b):
        block = second.at[pl.ds(2 * own, 2), group(g), b]
        remote(block, block, zs_s.at[0], zs_r.at[g * 2 + b], partner).wait_recv()

    def ring_copy(g, w, t, arrival=0):
        way = WAYS[w]
        m = lax.rem(step_y(-way * (t - 1 + arrival)), 4)
        block = second.at[pl.ds(2 * m, 2), group(g)] if t == 1 else second.at[2 * m + w, group(g)]
        n = (g * 2 + w) * 2 + t - 1
        return (block, block, ring_s.at[n], ring_r.at[n], device(step_y(way), zl, chip, core))

    def ring_second():
        for g in range(GROUPS):
            for w in range(2):
                remote(*ring_copy(g, w, 1, 1)).wait_recv()
                send(*ring_copy(g, w, 2))

    def ring_end():
        for g in range(GROUPS):
            for w in range(2):
                remote(*ring_copy(g, w, 2, 1)).wait_recv()

    def ring_first(g):
        @pl.when(holder)
        def _():
            spread_arrival(g, 1 - lax.rem(held, 2))

        @pl.when(jnp.logical_not(holder))
        def _():
            spread_arrival(g, 0)
            spread_arrival(g, 1)

        for w in range(2):
            send(*ring_copy(g, w, 1))

    spread(0)
    spread(1)
    block = first.at[far, :, eight(core), :]
    remote(mine, block, hi_s, hi_r, partner).wait_recv()
    for n in range(3):
        send(block, block, x_s.at[n + 3], x_r.at[n + 3], row_chips[n])

    ring_first(0)
    to_partner(0)
    ring_first(1)
    to_partner(1)

    lane = lax.broadcasted_iota(jnp.int32, (1, K), 1)
    sign = jnp.where(lane < K // 2, 1.0, -1.0).astype(F32)

    def build_rows(f):
        v = first[:, f].reshape(128, K)
        rows_v[f, 0] = v
        rows_v[f, 1] = (pltpu.roll(v.astype(F32), K // 2, 1) * sign).astype(BF)

    def compute(pairs):
        def one(f):
            rows = rows_v[f].reshape(256, K)
            cols = jnp.concatenate(
                [second[pl.ds(2 * m, 2), f, b].reshape(32, K) for m in pairs for b in range(2)], axis=0
            )
            twice = 1 if len(pairs) > 1 else 2
            cols = jnp.concatenate([cols] * twice, axis=0)
            cross = lax.dot_general(cols, rows, (((1,), (1,)), ((), ())), preferred_element_type=F32)
            blocks = []
            for n, m in enumerate(pairs):
                for b in range(2):
                    at = (2 * n + b) * 32
                    scale = scale_t[f, b, m].astype(F32)
                    block = [
                        (scale * (cross[at : at + 32, 128 * c : 128 * c + 128] - obs_t[f, c, b, m].astype(F32))).astype(BF)
                        for c in range(2)
                    ]
                    blocks.append(jnp.concatenate(block, axis=1))
                    res_t[f, b, m] = blocks[-1]
            gs = jnp.dot(jnp.concatenate(blocks * twice, axis=0), rows, preferred_element_type=F32)
            for n, m in enumerate(pairs):
                for b in range(2):
                    at = (2 * n + b) * 32
                    gs_own[4 * b + m, f] = gs[at : at + 32].astype(BF)

        over(0, F, one)

    def first_gradient(f):
        residual = res_t[f].reshape(256, 256)
        cols = jnp.concatenate([second[:, f, b].reshape(128, K) for b in range(2)], axis=0)
        prod = lax.dot_general(residual, cols, (((0,), (0,)), ((), ())), preferred_element_type=F32)
        gf = prod[:128] - pltpu.roll(prod[128:], K // 2, 1) * sign
        gf = gf.reshape(CHIPS, 2, 8, K)
        for c in range(2):
            gf_own[c, :, f] = gf[:, c].astype(BF)

    def red_copy(g, w, t):
        way = WAYS[w]
        n = MESSAGE[g, w, t]
        src = gs_own.at[step_y(way * (steps_of(g, w) - t + 1)), group(g)]
        return (src, gs_got.at[n], red_s.at[n], red_r.at[n], device(step_y(way), zl, chip, core))

    def reduce(distance, start=0, stop=GROUPS):
        for g in range(start, stop):
            for w in range(2):
                t = steps_of(g, w) - distance + 1
                if t < 1:
                    continue
                if t > 1:
                    remote(*red_copy(g, w, t - 1)).wait_recv()
                    acc = gs_own.at[step_y(WAYS[w] * distance), group(g)]
                    acc[...] = (acc[...].astype(F32) + gs_got[MESSAGE[g, w, t - 1]].astype(F32)).astype(BF)
                send(*red_copy(g, w, t))

    def reduced(g):
        total = gs_own[y, group(g)].astype(F32)
        for w in range(2):
            steps = steps_of(g, w)
            remote(*red_copy(g, w, steps)).wait_recv()
            total = total + gs_got[MESSAGE[g, w, steps]].astype(F32)
        total = total.reshape(G, ZS, 8, K)
        for n in range(ZS):
            gz_own[n, group(g)] = total[:, n].astype(BF)
        for n in range(3):
            send(*z_copy(g, n))

    def z_copy(g, n):
        to = lax.rem(zl + n + 1, ZS)
        m = g * 3 + n
        return (gz_own.at[to, group(g)], gz_in.at[n, group(g)], z_s.at[m], z_r.at[m], z_line[n])

    def gf_pair(n):
        return (gf_own.at[1 - core, :, half(n)], gf_got.at[:, half(n)], gp_s.at[n], gp_r.at[n], partner)

    def gf_x(n, m):
        to = lax.rem(x + m + 1, 4)
        return (gf_sum.at[:, to, half(n)], gf_in.at[m, :, half(n)], gx_s.at[n * 3 + m], gx_r.at[n * 3 + m], row_chips[m])

    def gf_hi(n):
        return (gh_own.at[1 - hi, half(n)], gh_in.at[half(n)], gh_s.at[n], gh_r.at[n], device(y, zl, far, core))

    def gf_along_x(n):
        remote(*gf_pair(n)).wait_recv()
        value = gf_own[core, :, half(n)].astype(F32) + gf_got[:, half(n)].astype(F32)
        gf_sum[:, :, half(n)] = value.astype(BF).reshape(2, 4, HALF, 8, K)
        for m in range(3):
            send(*gf_x(n, m))

    def gf_across(n):
        value = gf_sum[:, x, half(n)].astype(F32)
        for m in range(3):
            remote(*gf_x(n, m)).wait_recv()
            value = value + gf_in[m, :, half(n)].astype(F32)
        gh_own[:, half(n)] = value.astype(BF)
        send(*gf_hi(n))

    for n in range(2):
        z_hi = hi if n == 0 else lax.rem(hi + 1, 2)
        block = first.at[pl.ds(z_hi * 4, 4), :, eight(1 - core), :]
        remote(block, block, pair_s.at[n], pair_r.at[n], partner).wait_recv()
    over(0, F, build_rows)
    compute([own])
    reduce(4)
    ring_second()
    compute([lax.rem(y + 1, 4), lax.rem(y + 3, 4)])
    reduce(3)
    ring_end()
    compute([lax.rem(y + 2, 4)])
    over(0, HALF, first_gradient)
    send(*gf_pair(0))
    reduce(2)
    over(HALF, F, first_gradient)
    send(*gf_pair(1))
    gf_along_x(0)
    reduce(1, 0, 1)
    gf_along_x(1)
    reduce(1, 1, 2)
    gf_across(0)
    reduced(0)
    gf_across(1)
    reduced(1)

    def put_out(value, out):
        turn[...] = value.reshape(8 * F, K)
        for s in range(8):
            out[s] = turn[pl.ds(s, F, stride=8), :].astype(BF)

    for n in range(2):
        remote(*gf_hi(n)).wait_recv()
    put_out(gh_own[hi].astype(F32) + gh_in[...].astype(F32), out.at[0])

    value = gz_own[zl].astype(F32)
    for n in range(3):
        for g in range(GROUPS):
            remote(*z_copy(g, n)).wait_recv()
        value = value + gz_in[n].astype(F32)
    put_out(value, out.at[1])

    for copy in sent:
        copy.wait_send()
    for n in range(2):

        @functools.partial(unless_stays, y // 4 == n)
        def _():
            for g in range(GROUPS):
                put(g, n).wait_send()


    @pl.when(holder)
    def _():
        for g in range(GROUPS):
            for copy in spread_copies(g):
                copy.wait_send()


def finish(both, grad_first, grad_second):
    grad_first[...] = both[0]
    grad_second[0] = both[1]


def per_device(spectra, window_flags, pair_mask, misfit_weight, observed):
    dma = pltpu.SemaphoreType.DMA
    vmem = pltpu.VMEM
    both = pl.pallas_call(
        kernel,
        out_shape=jax.ShapeDtypeStruct((2, 8, F, K), BF),
        in_specs=[pl.BlockSpec(memory_space=pl.ANY)] * 5,
        out_specs=pl.BlockSpec(memory_space=pltpu.VMEM),
        scratch_shapes=[
            vmem((8, F, K), BF),
            vmem((8, K // 2), jnp.int32),
            vmem((128, 256), jnp.int32),
            vmem((F, 128, 256), BF),
            vmem((2, F, 128, 256), BF),
            vmem((8 * F, K), F32),
            vmem((F, 8, K), BF),
            vmem((CHIPS, F, 16, K), BF),
            vmem((CHIPS, F, 2, 16, K), BF),
            vmem((F, 2, 4, 32, 128), BF),
            vmem((F, 2, 2, 4, 32, 128), BF),
            vmem((F, 2, 128, K), BF),
            vmem((F, 2, 4, 32, 256), BF),
            vmem((2, CHIPS, F, 8, K), BF),
            vmem((CHIPS, F, 8, K), BF),
            vmem((2, 4, F, 8, K), BF),
            vmem((3, 2, F, 8, K), BF),
            vmem((2, F, 8, K), BF),
            vmem((F, 8, K), BF),
            vmem((YS, F, 32, K), BF),
            vmem((MESSAGES, G, 32, K), BF),
            vmem((ZS, F, 8, K), BF),
            vmem((ZS - 1, F, 8, K), BF),
            dma((5,)),
            dma((2 * GROUPS,)), dma((4 * GROUPS,)),
            dma((3 * GROUPS,)), dma((2 * GROUPS,)),
            dma, dma,
            dma((6,)), dma((6,)),
            dma((2,)), dma((2,)),
            dma((4 * GROUPS,)), dma((4 * GROUPS,)),
            dma((2,)), dma((2,)),
            dma((6,)), dma((6,)),
            dma((2,)), dma((2,)),
            dma((MESSAGES,)), dma((MESSAGES,)),
            dma((3 * GROUPS,)), dma((3 * GROUPS,)),
        ],
        compiler_params=pltpu.CompilerParams(collective_id=0, has_side_effects=True),
    )(spectra, window_flags, pair_mask, misfit_weight, observed)
    return pl.pallas_call(
        finish,
        out_shape=(
            jax.ShapeDtypeStruct((8, F, K), BF),
            jax.ShapeDtypeStruct((1, 8, F, K), BF),
        ),
        in_specs=[pl.BlockSpec(memory_space=pltpu.VMEM)],
        out_specs=[pl.BlockSpec(memory_space=pltpu.VMEM)] * 2,
    )(both)


def solution(mesh):
    placed = (
        P(("row", "col"), None, None),
        P(("row", "col"), None),
        P("row", "col"),
        P(None, "row", "col"),
        P(None, None, "row", "col"),
    )
    return jax.shard_map(
        per_device,
        mesh=mesh,
        in_specs=placed,
        out_specs=(P(("row", "col"), None, None), P("col", "row", None, None)),
        check_vma=False,
    )
```

```python
import functools

import jax
import jax.numpy as jnp
from jax import lax
from jax.experimental import pallas as pl
from jax.experimental.pallas import tpu as pltpu
from jax.sharding import PartitionSpec as P

MESH = pl.DeviceIdType.MESH
BF = jnp.bfloat16
F32 = jnp.float32
F = 16
K = 128
CHIPS = 8
YS = 8
ZS = 4
GROUPS = 2
G = F // GROUPS
HALF = F // 2
UNROLL = 16
WAYS = (1, -1)


def steps_of(group, way):
    return 4 if (group + way) % 2 == 0 else 3


MESSAGE = {}
for _g in range(GROUPS):
    for _w in range(2):
        for _t in range(1, steps_of(_g, _w) + 1):
            MESSAGE[_g, _w, _t] = len(MESSAGE)
MESSAGES = len(MESSAGE)


def landing(zl, chip, other):
    mirrored = lax.rem(chip // 4 + other // 4, 2)
    return mirrored * (ZS - 1 - zl) + (1 - mirrored) * zl


def kernel(
    spectra, flags, mask, weight, observed, out,
    spec_v, flag_v, mask_v, weight_v, obs_v, turn, mine, first, second,
    scale_t, obs_t, rows_v, res_t,
    gf_own, gf_got, gf_sum, gf_in, gh_own, gh_in, gs_own, gs_got, gz_own, gz_in,
    load_sem, put_s, put_r, zs_s, zs_r, hi_s, hi_r, x_s, x_r, pair_s, pair_r, ring_s, ring_r,
    gp_s, gp_r, gx_s, gx_r, gh_s, gh_r, red_s, red_r, z_s, z_r,
):
    row = lax.axis_index("row")
    col = lax.axis_index("col")
    y, zl = row // ZS, lax.rem(row, ZS)
    chip, core = col // 2, lax.rem(col, 2)
    hi, x = chip // 4, lax.rem(chip, 4)

    def device(y, zl, chip, core):
        return (y * ZS + zl, chip * 2 + core)

    def step_y(n):
        return lax.rem(y + n + 2 * YS, YS)

    sent = []

    def remote(src, dst, send, recv, to):
        return pltpu.make_async_remote_copy(
            src_ref=src, dst_ref=dst, send_sem=send, recv_sem=recv, device_id=to, device_id_type=MESH
        )

    def send(*args):
        sent.append(remote(*args))
        sent[-1].start()

    def group(g):
        return slice(g * G, g * G + G)

    def half(n):
        return slice(n * HALF, n * HALF + HALF)

    def eight(c):
        return pl.ds(pl.multiple_of(c * 8, 8), 8)

    loads = [
        pltpu.make_async_copy(a, b, load_sem.at[n])
        for n, (a, b) in enumerate(
            ((spectra, spec_v), (flags, flag_v), (mask, mask_v), (weight, weight_v), (observed, obs_v))
        )
    ]
    loads[0].start()
    loads[1].start()

    barrier = pltpu.get_barrier_semaphore()
    partner = device(y, zl, chip, 1 - core)
    far = lax.rem(hi + 1, 2) * 4 + x
    own = lax.rem(y, 4)
    held = landing(zl, chip, 2 * own)
    holder = held // 2 == core
    stays = jnp.logical_and(jnp.logical_and(chip == y, chip // 2 == own), zl // 2 == core)
    my_piece = lax.rem(chip, 2) * 2 + core

    def unless_stays(is_it, body):
        pl.when(jnp.logical_not(jnp.logical_and(stays, is_it)))(body)

    block_chips = [lax.rem(chip + n, CHIPS) for n in (4, 5, 3, 6, 2, 7, 1)]
    row_chips = [device(y, zl, hi * 4 + lax.rem(x + n, 4), core) for n in range(1, 4)]
    z_line = [device(y, lax.rem(zl + n, ZS), chip, core) for n in range(1, ZS)]
    peers = [partner] + [device(y, zl, to, core) for to in block_chips] + z_line
    peers += [device(step_y(way), zl, chip, core) for way in WAYS]
    for peer in peers:
        pl.semaphore_signal(barrier, inc=1, device_id=peer, device_id_type=MESH)

    @pl.when(holder)
    def _():
        for n in range(4):

            @functools.partial(unless_stays, my_piece == n)
            def _():
                giver = device(chip, held, 2 * own + n // 2, n % 2)
                pl.semaphore_signal(barrier, inc=1, device_id=giver, device_id_type=MESH)

    for load in loads[2:]:
        load.start()

    loads[0].wait()
    loads[1].wait()
    turn[...] = spec_v[...].astype(F32).reshape(8 * F, K)
    flag = flag_v[...].astype(F32)
    flag = jnp.concatenate([flag, flag], axis=1)
    pieces = [(turn[pl.ds(f, 8, stride=F), :] * flag).astype(BF) for f in range(F)]
    for f in range(F):
        mine[f] = pieces[f]

    for c in range(2):

        @pl.when(core == c)
        def _():
            for f in range(F):
                first[chip, f, 8 * c : 8 * c + 8, :] = pieces[f]

            @pl.when(stays)
            def _():
                for f in range(F):
                    second[chip, f, lax.rem(zl, 2), 8 * c : 8 * c + 8, :] = pieces[f]

    @pl.when(stays)
    def _():
        pl.semaphore_wait(barrier, len(peers) + 1)

    @functools.partial(unless_stays, True)
    def _():
        pl.semaphore_wait(barrier, len(peers) + 2)


    def put(g, n):
        to = device(chip // 2 + 4 * n, landing(zl, chip, y), y, zl // 2)
        dst = second.at[chip, group(g), lax.rem(zl, 2), eight(core), :]
        return remote(mine.at[group(g)], dst, put_s.at[g * 2 + n], put_r.at[g * 4 + my_piece], to)

    for g in range(GROUPS):
        for n in range(2):

            @functools.partial(unless_stays, y // 4 == n)
            def _():
                put(g, n).start()

    send(mine, first.at[chip, :, eight(core), :], hi_s, hi_r, device(y, zl, far, core))
    for n in range(3):
        send(mine, first.at[chip, :, eight(core), :], x_s.at[n], x_r.at[n], row_chips[n])

    for load in loads[2:]:
        load.wait()

    def over(first_f, last_f, body):
        def several(n, carry):
            for m in range(min(UNROLL, last_f - first_f)):
                body(first_f + n * min(UNROLL, last_f - first_f) + m)
            return carry

        lax.fori_loop(0, (last_f - first_f) // min(UNROLL, last_f - first_f), several, 0)

    def prepare(f):
        scale = mask_v[...].astype(F32).astype(BF) * weight_v[f]
        scale_t[f] = scale.T.reshape(2, 4, 32, 128)
        for c in range(2):
            obs_t[f, c] = obs_v[c, f].T.reshape(2, 4, 32, 128)

    over(0, F, prepare)

    def spread_copies(g):
        block = second.at[pl.ds(2 * own, 2), group(g), lax.rem(held, 2)]
        return [
            remote(block, block, zs_s.at[g * 3 + n], zs_r.at[g * 2 + lax.rem(held, 2)], z_line[n]) for n in range(3)
        ]

    def spread(g):
        @pl.when(holder)
        def _():
            for n in range(4):

                @functools.partial(unless_stays, my_piece == n)
                def _():
                    c = n % 2
                    block = second.at[2 * own + n // 2, group(g), lax.rem(held, 2), 8 * c : 8 * c + 8, :]
                    remote(mine.at[group(g)], block, put_s.at[0], put_r.at[g * 4 + n], partner).wait_recv()

            for copy in spread_copies(g):
                copy.start()


    def to_partner(n):
        z_hi = hi if n == 0 else lax.rem(hi + 1, 2)
        for m in range(3):
            from_chip = z_hi * 4 + lax.rem(x - m - 1 + 4, 4)
            remote(
                mine, first.at[from_chip, :, eight(core), :], x_s.at[0], x_r.at[n * 3 + m], partner
            ).wait_recv()
        block = first.at[pl.ds(z_hi * 4, 4), :, eight(core), :]
        send(block, block, pair_s.at[n], pair_r.at[n], partner)


    def spread_arrival(g, b):
        block = second.at[pl.ds(2 * own, 2), group(g), b]
        remote(block, block, zs_s.at[0], zs_r.at[g * 2 + b], partner).wait_recv()

    def ring_copy(g, w, t, arrival=0):
        way = WAYS[w]
        m = lax.rem(step_y(-way * (t - 1 + arrival)), 4)
        block = second.at[pl.ds(2 * m, 2), group(g)] if t == 1 else second.at[2 * m + w, group(g)]
        n = (g * 2 + w) * 2 + t - 1
        return (block, block, ring_s.at[n], ring_r.at[n], device(step_y(way), zl, chip, core))

    def ring_second():
        for g in range(GROUPS):
            for w in range(2):
                remote(*ring_copy(g, w, 1, 1)).wait_recv()
                send(*ring_copy(g, w, 2))

    def ring_end():
        for g in range(GROUPS):
            for w in range(2):
                remote(*ring_copy(g, w, 2, 1)).wait_recv()

    def ring_first(g):
        @pl.when(holder)
        def _():
            spread_arrival(g, 1 - lax.rem(held, 2))

        @pl.when(jnp.logical_not(holder))
        def _():
            spread_arrival(g, 0)
            spread_arrival(g, 1)

        for w in range(2):
            send(*ring_copy(g, w, 1))

    spread(0)
    spread(1)
    block = first.at[far, :, eight(core), :]
    remote(mine, block, hi_s, hi_r, partner).wait_recv()
    for n in range(3):
        send(block, block, x_s.at[n + 3], x_r.at[n + 3], row_chips[n])

    ring_first(0)
    to_partner(0)
    ring_first(1)
    to_partner(1)

    lane = lax.broadcasted_iota(jnp.int32, (1, K), 1)
    sign = jnp.where(lane < K // 2, 1.0, -1.0).astype(F32)

    def build_rows(f):
        v = first[:, f].reshape(128, K)
        rows_v[f, 0] = v
        rows_v[f, 1] = (pltpu.roll(v.astype(F32), K // 2, 1) * sign).astype(BF)

    def compute(pairs):
        def one(f):
            rows = rows_v[f].reshape(256, K)
            cols = jnp.concatenate(
                [second[pl.ds(2 * m, 2), f, b].reshape(32, K) for m in pairs for b in range(2)], axis=0
            )
            twice = 1 if len(pairs) > 1 else 2
            cols = jnp.concatenate([cols] * twice, axis=0)
            cross = lax.dot_general(cols, rows, (((1,), (1,)), ((), ())), preferred_element_type=F32)
            blocks = []
            for n, m in enumerate(pairs):
                for b in range(2):
                    at = (2 * n + b) * 32
                    scale = scale_t[f, b, m].astype(F32)
                    block = [
                        (scale * (cross[at : at + 32, 128 * c : 128 * c + 128] - obs_t[f, c, b, m].astype(F32))).astype(BF)
                        for c in range(2)
                    ]
                    blocks.append(jnp.concatenate(block, axis=1))
                    res_t[f, b, m] = blocks[-1]
            gs = jnp.dot(jnp.concatenate(blocks * twice, axis=0), rows, preferred_element_type=F32)
            for n, m in enumerate(pairs):
                for b in range(2):
                    at = (2 * n + b) * 32
                    gs_own[4 * b + m, f] = gs[at : at + 32].astype(BF)

        over(0, F, one)

    def first_gradient(f):
        residual = res_t[f].reshape(256, 256)
        cols = jnp.concatenate([second[:, f, b].reshape(128, K) for b in range(2)], axis=0)
        prod = lax.dot_general(residual, cols, (((0,), (0,)), ((), ())), preferred_element_type=F32)
        gf = prod[:128] - pltpu.roll(prod[128:], K // 2, 1) * sign
        gf = gf.reshape(CHIPS, 2, 8, K)
        for c in range(2):
            gf_own[c, :, f] = gf[:, c].astype(BF)

    def red_copy(g, w, t):
        way = WAYS[w]
        n = MESSAGE[g, w, t]
        src = gs_own.at[step_y(way * (steps_of(g, w) - t + 1)), group(g)]
        return (src, gs_got.at[n], red_s.at[n], red_r.at[n], device(step_y(way), zl, chip, core))

    def reduce(distance, start=0, stop=GROUPS):
        for g in range(start, stop):
            for w in range(2):
                t = steps_of(g, w) - distance + 1
                if t < 1:
                    continue
                if t > 1:
                    remote(*red_copy(g, w, t - 1)).wait_recv()
                    acc = gs_own.at[step_y(WAYS[w] * distance), group(g)]
                    acc[...] = (acc[...].astype(F32) + gs_got[MESSAGE[g, w, t - 1]].astype(F32)).astype(BF)
                send(*red_copy(g, w, t))

    def reduced(g):
        total = gs_own[y, group(g)].astype(F32)
        for w in range(2):
            steps = steps_of(g, w)
            remote(*red_copy(g, w, steps)).wait_recv()
            total = total + gs_got[MESSAGE[g, w, steps]].astype(F32)
        total = total.reshape(G, ZS, 8, K)
        for n in range(ZS):
            gz_own[n, group(g)] = total[:, n].astype(BF)
        for n in range(3):
            send(*z_copy(g, n))

    def z_copy(g, n):
        to = lax.rem(zl + n + 1, ZS)
        m = g * 3 + n
        return (gz_own.at[to, group(g)], gz_in.at[n, group(g)], z_s.at[m], z_r.at[m], z_line[n])

    def gf_pair(n):
        return (gf_own.at[1 - core, :, half(n)], gf_got.at[:, half(n)], gp_s.at[n], gp_r.at[n], partner)

    def gf_x(n, m):
        to = lax.rem(x + m + 1, 4)
        return (gf_sum.at[:, to, half(n)], gf_in.at[m, :, half(n)], gx_s.at[n * 3 + m], gx_r.at[n * 3 + m], row_chips[m])

    def gf_hi(n):
        return (gh_own.at[1 - hi, half(n)], gh_in.at[half(n)], gh_s.at[n], gh_r.at[n], device(y, zl, far, core))

    def gf_along_x(n):
        remote(*gf_pair(n)).wait_recv()
        value = gf_own[core, :, half(n)].astype(F32) + gf_got[:, half(n)].astype(F32)
        gf_sum[:, :, half(n)] = value.astype(BF).reshape(2, 4, HALF, 8, K)
        for m in range(3):
            send(*gf_x(n, m))

    def gf_across(n):
        value = gf_sum[:, x, half(n)].astype(F32)
        for m in range(3):
            remote(*gf_x(n, m)).wait_recv()
            value = value + gf_in[m, :, half(n)].astype(F32)
        gh_own[:, half(n)] = value.astype(BF)
        send(*gf_hi(n))

    for n in range(2):
        z_hi = hi if n == 0 else lax.rem(hi + 1, 2)
        block = first.at[pl.ds(z_hi * 4, 4), :, eight(1 - core), :]
        remote(block, block, pair_s.at[n], pair_r.at[n], partner).wait_recv()
    over(0, F, build_rows)
    compute([own])
    reduce(4)
    ring_second()
    compute([lax.rem(y + 1, 4), lax.rem(y + 3, 4)])
    reduce(3)
    ring_end()
    compute([lax.rem(y + 2, 4)])
    reduce(2)
    over(0, HALF, first_gradient)
    send(*gf_pair(0))
    over(HALF, F, first_gradient)
    send(*gf_pair(1))
    gf_along_x(0)
    reduce(1, 0, 1)
    gf_along_x(1)
    reduce(1, 1, 2)
    gf_across(0)
    reduced(0)
    gf_across(1)
    reduced(1)

    def put_out(value, out):
        turn[...] = value.reshape(8 * F, K)
        for s in range(8):
            out[s] = turn[pl.ds(s, F, stride=8), :].astype(BF)

    for n in range(2):
        remote(*gf_hi(n)).wait_recv()
    put_out(gh_own[hi].astype(F32) + gh_in[...].astype(F32), out.at[0])

    value = gz_own[zl].astype(F32)
    for n in range(3):
        for g in range(GROUPS):
            remote(*z_copy(g, n)).wait_recv()
        value = value + gz_in[n].astype(F32)
    put_out(value, out.at[1])

    for copy in sent:
        copy.wait_send()
    for n in range(2):

        @functools.partial(unless_stays, y // 4 == n)
        def _():
            for g in range(GROUPS):
                put(g, n).wait_send()


    @pl.when(holder)
    def _():
        for g in range(GROUPS):
            for copy in spread_copies(g):
                copy.wait_send()


def finish(both, grad_first, grad_second):
    grad_first[...] = both[0]
    grad_second[0] = both[1]


def per_device(spectra, window_flags, pair_mask, misfit_weight, observed):
    dma = pltpu.SemaphoreType.DMA
    vmem = pltpu.VMEM
    both = pl.pallas_call(
        kernel,
        out_shape=jax.ShapeDtypeStruct((2, 8, F, K), BF),
        in_specs=[pl.BlockSpec(memory_space=pl.ANY)] * 5,
        out_specs=pl.BlockSpec(memory_space=pltpu.VMEM),
        scratch_shapes=[
            vmem((8, F, K), BF),
            vmem((8, K // 2), jnp.int32),
            vmem((128, 256), jnp.int32),
            vmem((F, 128, 256), BF),
            vmem((2, F, 128, 256), BF),
            vmem((8 * F, K), F32),
            vmem((F, 8, K), BF),
            vmem((CHIPS, F, 16, K), BF),
            vmem((CHIPS, F, 2, 16, K), BF),
            vmem((F, 2, 4, 32, 128), BF),
            vmem((F, 2, 2, 4, 32, 128), BF),
            vmem((F, 2, 128, K), BF),
            vmem((F, 2, 4, 32, 256), BF),
            vmem((2, CHIPS, F, 8, K), BF),
            vmem((CHIPS, F, 8, K), BF),
            vmem((2, 4, F, 8, K), BF),
            vmem((3, 2, F, 8, K), BF),
            vmem((2, F, 8, K), BF),
            vmem((F, 8, K), BF),
            vmem((YS, F, 32, K), BF),
            vmem((MESSAGES, G, 32, K), BF),
            vmem((ZS, F, 8, K), BF),
            vmem((ZS - 1, F, 8, K), BF),
            dma((5,)),
            dma((2 * GROUPS,)), dma((4 * GROUPS,)),
            dma((3 * GROUPS,)), dma((2 * GROUPS,)),
            dma, dma,
            dma((6,)), dma((6,)),
            dma((2,)), dma((2,)),
            dma((4 * GROUPS,)), dma((4 * GROUPS,)),
            dma((2,)), dma((2,)),
            dma((6,)), dma((6,)),
            dma((2,)), dma((2,)),
            dma((MESSAGES,)), dma((MESSAGES,)),
            dma((3 * GROUPS,)), dma((3 * GROUPS,)),
        ],
        compiler_params=pltpu.CompilerParams(collective_id=0, has_side_effects=True),
    )(spectra, window_flags, pair_mask, misfit_weight, observed)
    return pl.pallas_call(
        finish,
        out_shape=(
            jax.ShapeDtypeStruct((8, F, K), BF),
            jax.ShapeDtypeStruct((1, 8, F, K), BF),
        ),
        in_specs=[pl.BlockSpec(memory_space=pltpu.VMEM)],
        out_specs=[pl.BlockSpec(memory_space=pltpu.VMEM)] * 2,
    )(both)


def solution(mesh):
    placed = (
        P(("row", "col"), None, None),
        P(("row", "col"), None),
        P("row", "col"),
        P(None, "row", "col"),
        P(None, None, "row", "col"),
    )
    return jax.shard_map(
        per_device,
        mesh=mesh,
        in_specs=placed,
        out_specs=(P(("row", "col"), None, None), P("col", "row", None, None)),
        check_vma=False,
    )
```
